32 devices in a mesh: gz: 2 (over core), pa: 16 (over z, y, x).
Axes of the slice: x: 2, y: 2, z: 4, core: 2. Of those that a mesh axis runs over, the one named last changes fastest.
Arguments:
- velocity: float32 [3, 2, 2, 512, 1024], P(None, 'gz', None, 'pa'), may hold values from -3 to 3
- mode_mask: int32 [512, 1024], P('pa'), may hold values from 0 to 1, as said below
Outputs:
- velocity_next: float32 [3, 2, 2, 512, 1024], P(None, 'gz', None, 'pa')
- divergence: float32 [2, 2, 512, 1024], P('gz', None, 'pa')
The draws below stay inside these ranges and needn't reach their ends.
Inputs may be any that keep to these rules, and one draw needn't show every extreme that they name: mode_mask is 1 exactly where |s(m)| <= A and n <= B, for one A from 256 to 340 and one B from 256 to 340 in each draw, and 0 elsewhere.
All inputs are finite; a program needn't handle non-finite values.
Results may differ from the reference program's by a relative error of at most 0.00005.
Values sent between devices are 32-bit elements; how exact they have to be, the bound alone decides.
No kernel may reach another device: no remote copies, remote signals or barrier semaphores. Data moves between devices by JAX's collectives and lax.ppermute only.
A program may use at most 64 MiB of HBM per device.

```python
import math
import jax
import jax.numpy as jnp
from jax import lax

NX = 1024
NY = 1024
NZ = 2
KY = 512


def draw_mode_mask(key, part):
    first_key = jax.random.fold_in(key, 11)
    second_key = jax.random.fold_in(key, 23)
    cut_x = jax.random.randint(first_key, (), NX // 4, NX // 3)
    cut_y = jax.random.randint(second_key, (), NY // 4, NY // 3)
    modes = jnp.arange(NX, dtype=jnp.int32)
    signed = jnp.where(modes < NX // 2, modes, modes - NX)
    spanwise = jnp.arange(NY // 2, dtype=jnp.int32)
    inside = (jnp.abs(signed)[None, :] <= cut_x) & (spanwise[:, None] <= cut_y)
    return inside.astype(jnp.int32)


def shard_levels(stream_key, dims, shards, low, high):
    gain = 1.0
    for position, blocks in shards:
        steps = jax.random.uniform(jax.random.fold_in(jax.random.fold_in(stream_key, 6), position), (blocks,), jnp.float32, low / len(shards), high / len(shards))
        gain = gain * jnp.repeat(jnp.exp(steps), dims[position] // blocks).reshape((-1,) + (1,) * (len(dims) - 1 - position))
    return gain


def gaussian(key, shape, width, limit, shards=(), kind=jnp.bfloat16):
    factor_of = shard_levels(key, shape, shards, -0.22, 0.18) if shards else 1.0
    drawn = jax.random.normal(key, shape, jnp.float32) * width * factor_of
    return jnp.minimum(jnp.maximum(drawn, -limit), limit).astype(kind)


def setup_inputs(seed: int = 0) -> dict:
    keys = jax.random.split(jax.random.key(seed), 3)
    velocity = gaussian(keys[0], (3, NZ, 2, KY, NX), 0.5, 3.0, ((1, 2), (3, 16)), jnp.float32)
    mode_mask = draw_mode_mask(jax.random.fold_in(keys[2], 71), 0)
    return dict(velocity=velocity, mode_mask=mode_mask)


def wall_first(padded):
    return 0.5 * (padded[2:] - padded[:-2])


def times_wave(wave, field):
    return jnp.stack([-wave * field[:, 1], wave * field[:, 0]], 1)


def reference(velocity, mode_mask):
    half = NY // 2
    modes = jnp.arange(NX, dtype=jnp.int32)
    signed = jnp.where(modes < NX // 2, modes, modes - NX)
    kx_wave = (2.0 * math.pi / NX) * signed.astype(jnp.float32)
    ky_wave = ((2.0 * math.pi / NY) * jnp.arange(half, dtype=jnp.int32).astype(jnp.float32))[:, None]
    padded = jnp.pad(velocity, ((0, 0), (1, 1), (0, 0), (0, 0), (0, 0)))
    u_spec, v_spec, w_spec = velocity[0], velocity[1], velocity[2]
    omega_x = times_wave(ky_wave, w_spec) - wall_first(padded[1])
    omega_y = wall_first(padded[0]) - times_wave(kx_wave, w_spec)
    omega_z = times_wave(kx_wave, v_spec) - times_wave(ky_wave, u_spec)
    spectral = jnp.concatenate([velocity, jnp.stack([omega_x, omega_y, omega_z], 0)], 0)

    def plane(spec):
        coeff = spec[:, 0] + 1j * spec[:, 1]
        columns = jnp.fft.ifft(coeff, axis=2, norm="ortho")
        full = jnp.concatenate([columns, jnp.zeros((6, 1, NX), columns.dtype)], axis=1)
        grid = jnp.fft.irfft(full, n=NY, axis=1, norm="ortho")
        u_grid, v_grid, w_grid, ox_grid, oy_grid, oz_grid = grid[0], grid[1], grid[2], grid[3], grid[4], grid[5]
        cross = jnp.stack([v_grid * oz_grid - w_grid * oy_grid,
                           w_grid * ox_grid - u_grid * oz_grid,
                           u_grid * oy_grid - v_grid * ox_grid], 0)
        rows = jnp.fft.rfft(cross, axis=1, norm="ortho")[:, :half]
        result = jnp.fft.fft(rows, axis=2, norm="ortho")
        return jnp.stack([result.real, result.imag], 1)

    nonlinear = lax.map(plane, jnp.moveaxis(spectral, 1, 0))
    nonlinear = jnp.moveaxis(nonlinear, 0, 1)
    mask = mode_mask.astype(jnp.float32)
    viscous = padded[:, 2:] - 2.0 * padded[:, 1:-1] + padded[:, :-2]
    viscous = viscous - (kx_wave * kx_wave + ky_wave * ky_wave) * velocity
    following = velocity + 0.2 * (nonlinear * mask + 0.25 * viscous)
    w_padded = jnp.pad(following[2], ((1, 1), (0, 0), (0, 0), (0, 0)))
    divergence = times_wave(kx_wave, following[0]) + times_wave(ky_wave, following[1]) + wall_first(w_padded)
    return following, divergence
```

```python
import functools
import math

import jax
import jax.numpy as jnp
import ml_dtypes
import numpy as np
from jax import lax
from jax.experimental import pallas as pl
from jax.experimental.pallas import tpu as pltpu
from jax.sharding import PartitionSpec as P

time_step = 0.2
viscosity = 0.25
LANES = 128
HALF = LANES // 2
ROWS = 8


def halves(table):
    high = table.astype(np.float32).astype(ml_dtypes.bfloat16)
    low = (table - high.astype(np.float64)).astype(np.float32).astype(ml_dtypes.bfloat16)
    return np.stack([high, low])


def wheel(rows, cols, period):
    angle = 2.0 * np.pi / period * (np.outer(rows, cols) % period)
    return np.cos(angle), np.sin(angle)


@functools.lru_cache(maxsize=None)
def tables(ncols, half, lines):
    radix = ncols // LANES
    lane = np.arange(LANES)
    scale = 1.0 / math.sqrt(ncols)
    cos, sin = wheel(lane, lane, LANES)
    forward = np.zeros((2 * LANES, 2 * LANES))
    for part in range(LANES // lines):
        x2 = np.arange(part * lines, (part + 1) * lines)
        at = part * 2 * lines
        forward[:LANES, at : at + lines] = cos[:, x2]
        forward[LANES:, at : at + lines] = -sin[:, x2]
        forward[:LANES, at + lines : at + 2 * lines] = sin[:, x2]
        forward[LANES:, at + lines : at + 2 * lines] = cos[:, x2]
    backward = forward.T
    turn_cos, turn_sin = wheel(np.arange(radix), lane, ncols)
    turns = np.concatenate([turn_cos, turn_sin]).astype(np.float32)
    quarter = half // 2
    nrows = 2 * half
    b = np.arange(quarter)
    yscale = 1.0 / math.sqrt(nrows)
    ycos, ysin = wheel(b, b, quarter)
    to_grid = 2.0 * yscale * np.concatenate([ycos, -ysin], 1)
    from_grid = yscale * np.concatenate([ycos, -ysin], 0)
    column = np.zeros((quarter, LANES))
    for y1 in range(1, 4):
        c, s = wheel(b, np.array([y1]), nrows)
        column[:, 2 * y1] = c[:, 0]
        column[:, 2 * y1 + 1] = s[:, 0]
    modes = np.arange(ncols)
    signed = np.where(modes < ncols // 2, modes, modes - ncols).astype(np.float32)
    wave = np.broadcast_to(np.float32(2.0 * math.pi / ncols) * signed, (ROWS, ncols))
    return dict(
        forward=halves(forward * scale),
        backward=halves(backward * scale),
        turns=turns,
        to_grid=halves(to_grid),
        from_grid=halves(from_grid),
        column=column.astype(np.float32),
        wave=np.ascontiguousarray(wave),
    )


def split(value):
    high = value.astype(jnp.bfloat16)
    low = (value - high.astype(jnp.float32)).astype(jnp.bfloat16)
    return high, low


def product(a_high, a_low, b_high, b_low):
    dot = functools.partial(jnp.dot, preferred_element_type=jnp.float32)
    return dot(a_high, b_low) + dot(a_low, b_high) + dot(a_high, b_high)


def butterfly(terms, sign):
    count = len(terms)
    if count == 1:
        return terms
    even = butterfly(terms[0::2], sign)
    odd = butterfly(terms[1::2], sign)
    first, second = [], []
    for k in range(count // 2):
        real, imag = odd[k]
        if k == 0:
            pass
        elif 4 * k == count:
            real, imag = -sign * imag, sign * real
        elif 8 * k == count:
            root = math.sqrt(0.5)
            real, imag = root * (real - sign * imag), root * (imag + sign * real)
        elif 8 * k == 3 * count:
            root = math.sqrt(0.5)
            real, imag = -root * (real + sign * imag), root * (sign * real - imag)
        else:
            c = math.cos(2.0 * math.pi * k / count)
            s = sign * math.sin(2.0 * math.pi * k / count)
            real, imag = c * real - s * imag, s * real + c * imag
        first.append((even[k][0] + real, even[k][1] + imag))
        second.append((even[k][0] - real, even[k][1] - imag))
    return first + second


def x_forward_kernel(vel_ref, wave_ref, turn_ref, mat_ref, out_ref, mid_ref):
    kyl, ncols = vel_ref.shape[2:]
    radix = ncols // LANES

    def chunk(c, carry):
        base = pl.multiple_of(c * ROWS, ROWS)
        rows = pl.ds(base, ROWS)

        def emit(field, terms):
            for x1, (real, imag) in enumerate(butterfly(terms, 1.0)):
                if x1:
                    cos = turn_ref[x1 : x1 + 1, :]
                    sin = turn_ref[radix + x1 : radix + x1 + 1, :]
                    real, imag = real * cos - imag * sin, real * sin + imag * cos
                at = pl.ds(pl.multiple_of(field * kyl + base, ROWS), ROWS)
                mid_ref[x1, at, 0:LANES] = real
                mid_ref[x1, at, LANES : 2 * LANES] = imag

        def load(field):
            cols = [slice(a * LANES, (a + 1) * LANES) for a in range(radix)]
            return [(vel_ref[field, 0, rows, s], vel_ref[field, 1, rows, s]) for s in cols]

        def slope(terms):
            waves = [wave_ref[:, a * LANES : (a + 1) * LANES] for a in range(radix)]
            return [(-k * imag, k * real) for k, (real, imag) in zip(waves, terms)]

        emit(0, load(0))
        emit(1, load(1))
        emit(2, load(2))
        emit(3, slope(load(2)))
        emit(4, slope(load(1)))
        return carry

    lax.fori_loop(0, kyl // ROWS, chunk, 0)
    for x1 in range(radix):
        high, low = split(mid_ref[x1])
        lines = product(high, low, mat_ref[0], mat_ref[1])
        out_ref[2 * x1] = lines[:, :LANES]
        out_ref[2 * x1 + 1] = lines[:, LANES:]


def grid_kernel(recv_ref, wall_ref, to_ref, from_ref, column_ref, out_ref, high_ref, low_ref, back_high, back_low):
    groups = recv_ref.shape[0]
    kyl = recv_ref.shape[1] // 5
    quarter = groups * kyl // 2
    block = 32
    each = block // kyl
    gap = groups // 2
    ky_step = 2.0 * math.pi / (4 * quarter)
    left = lax.broadcasted_iota(jnp.int32, (block, LANES), 1) < HALF
    swap = lambda value: pltpu.roll(value, HALF, 1)

    def fields(first, row):
        sources = pl.ds(first, each)
        load = lambda ref, f: ref[sources, f * kyl : (f + 1) * kyl, :].reshape(block, LANES)
        index = row + lax.broadcasted_iota(jnp.int32, (block, LANES), 0)
        ky = index.astype(jnp.float32) * ky_step
        weight = jnp.where(index == 0, 0.5, 1.0)
        ky_signed = jnp.where(left, -ky, ky)
        u, v, w, dw, dv = [load(recv_ref, f) for f in range(5)]
        du_dz, dv_dz = load(wall_ref, 0), load(wall_ref, 1)
        omega_x = ky_signed * swap(w) - dv_dz
        omega_y = du_dz - dw
        omega_z = dv - ky_signed * swap(u)
        result = []
        for one, two in ((u, v), (omega_x, omega_y), (w, omega_z)):
            one = one * weight
            two = two * weight
            result.append((jnp.where(left, one, swap(two)), jnp.where(left, swap(one), two)))
        return result

    def column(rows, k):
        return jnp.broadcast_to(column_ref[rows, k : k + 1], (block, LANES))

    def load_block(c, carry):
        base = pl.multiple_of(c * block, block)
        rows = pl.ds(base, block)
        near = fields(c * each, base)
        far = fields(c * each + gap, base + quarter)
        for pair in range(3):
            a_re, a_im = near[pair]
            b_re, b_im = far[pair]
            sums = (
                (a_re + b_re, a_im + b_im),
                (a_re - b_im, a_im + b_re),
                (a_re - b_re, a_im - b_im),
                (a_re + b_im, a_im - b_re),
            )
            for y1, (real, imag) in enumerate(sums):
                if y1:
                    cos = column(rows, 2 * y1)
                    sin = column(rows, 2 * y1 + 1)
                    real, imag = real * cos - imag * sin, real * sin + imag * cos
                at = slice((3 * y1 + pair) * LANES, (3 * y1 + pair + 1) * LANES)
                lower = pl.ds(pl.multiple_of(quarter + base, block), block)
                high_ref[rows, at], low_ref[rows, at] = split(real)
                high_ref[lower, at], low_ref[lower, at] = split(imag)
        return carry

    lax.fori_loop(0, quarter // block, load_block, 0)

    wide = lax.broadcasted_iota(jnp.int32, (quarter, LANES), 1) < HALF
    kept = None
    for y1 in range(4):
        at = slice(3 * y1 * LANES, 3 * (y1 + 1) * LANES)
        grid = product(to_ref[0], to_ref[1], high_ref[:, at], low_ref[:, at])
        uv = grid[:, :LANES]
        xy = grid[:, LANES : 2 * LANES]
        wz = grid[:, 2 * LANES :]
        zw = swap(wz)
        h_yx = jnp.where(wide, wz, zw) * xy - jnp.where(wide, zw, wz) * uv
        spin = uv * swap(xy)
        h_z = spin - swap(spin)
        slot = slice(y1 * LANES, (y1 + 1) * LANES)
        back_high[:, slot], back_low[:, slot] = split(h_yx)
        if y1 % 2 == 0:
            kept = h_z
        else:
            slot = slice((4 + y1 // 2) * LANES, (5 + y1 // 2) * LANES)
            back_high[:, slot], back_low[:, slot] = split(jnp.where(wide, kept, -h_z))

    freq = product(from_ref[0], from_ref[1], back_high[...], back_low[...])

    column_all = lambda k: jnp.broadcast_to(column_ref[:, k : k + 1], (quarter, LANES))

    def piece(slot, cos, sin):
        real = freq[:quarter, slot * LANES : (slot + 1) * LANES]
        imag = freq[quarter:, slot * LANES : (slot + 1) * LANES]
        if cos is None:
            return real, imag
        return real * cos + imag * sin, imag * cos - real * sin

    turn = [(None, None)] + [(column_all(2 * y1), column_all(2 * y1 + 1)) for y1 in range(1, 4)]
    one = jnp.ones((quarter, LANES), jnp.float32)
    zero = jnp.zeros((quarter, LANES), jnp.float32)
    q0, q1, q2, q3 = [piece(y1, *turn[y1]) for y1 in range(4)]
    z01 = piece(4, jnp.where(wide, one, turn[1][0]), jnp.where(wide, zero, turn[1][1]))
    z23 = piece(5, jnp.where(wide, turn[2][0], turn[3][0]), jnp.where(wide, turn[2][1], turn[3][1]))
    near_re = q0[0] + q1[0] + q2[0] + q3[0]
    near_im = q0[1] + q1[1] + q2[1] + q3[1]
    far_re = q0[0] + q1[1] - q2[0] - q3[1]
    far_im = q0[1] - q1[0] - q2[1] + q3[0]
    v_re, v_im = z01[0] + z23[0], z01[1] + z23[1]
    z_near = jnp.where(wide, v_re + swap(v_re), v_im + swap(v_im))
    d_re, d_im = z01[0] - z23[0], z01[1] - z23[1]
    z_far = jnp.where(wide, d_re + swap(d_im), swap(d_im) - d_re)

    def store(first, field, value):
        for s in range(gap):
            out_ref[first + s, field * kyl : (field + 1) * kyl, :] = value[s * kyl : (s + 1) * kyl]

    for first, real, imag, h_z in ((0, near_re, near_im, z_near), (gap, far_re, far_im, z_far)):
        store(first, 0, -jnp.where(wide, swap(real), imag))
        store(first, 1, jnp.where(wide, real, swap(imag)))
        store(first, 2, h_z)


def x_backward_kernel(recv_ref, vel_ref, side_ref, mask_ref, ky_ref, wave_ref, turn_ref, mat_ref, next_ref, div_ref, w_ref, mid_ref):
    kyl, ncols = vel_ref.shape[2:]
    radix = ncols // LANES
    for x1 in range(radix):
        high, low = split(jnp.concatenate([recv_ref[2 * x1], recv_ref[2 * x1 + 1]], axis=1))
        freq = product(high, low, mat_ref[0], mat_ref[1])
        real = freq[:, :LANES]
        imag = freq[:, LANES:]
        if x1:
            cos = turn_ref[x1 : x1 + 1, :]
            sin = turn_ref[radix + x1 : radix + x1 + 1, :]
            real, imag = real * cos + imag * sin, imag * cos - real * sin
        mid_ref[x1, :, 0:LANES] = real
        mid_ref[x1, :, LANES : 2 * LANES] = imag

    def chunk(c, carry):
        base = pl.multiple_of(c * ROWS, ROWS)
        rows = pl.ds(base, ROWS)
        ky = ky_ref[rows, :]
        for field in range(3):
            at = pl.ds(pl.multiple_of(field * kyl + base, ROWS), ROWS)
            terms = [(mid_ref[x1, at, 0:LANES], mid_ref[x1, at, LANES : 2 * LANES]) for x1 in range(radix)]
            for a, pair in enumerate(butterfly(terms, -1.0)):
                cols = slice(a * LANES, (a + 1) * LANES)
                kx = wave_ref[:, cols]
                keep = mask_ref[rows, cols] != 0
                decay = viscosity * (2.0 + kx * kx + ky * ky)
                fresh = []
                for part in range(2):
                    speed = vel_ref[field, part, rows, cols]
                    change = jnp.where(keep, pair[part], 0.0)
                    change = change + viscosity * side_ref[field, part, rows, cols] - decay * speed
                    fresh.append(speed + time_step * change)
                    next_ref[field, part, rows, cols] = fresh[part]
                if field == 0:
                    div_ref[0, rows, cols] = -kx * fresh[1]
                    div_ref[1, rows, cols] = kx * fresh[0]
                elif field == 1:
                    div_ref[0, rows, cols] = div_ref[0, rows, cols] - ky * fresh[1]
                    div_ref[1, rows, cols] = div_ref[1, rows, cols] + ky * fresh[0]
                else:
                    w_ref[0, rows, cols] = fresh[0]
                    w_ref[1, rows, cols] = fresh[1]
        return carry

    lax.fori_loop(0, kyl // ROWS, chunk, 0)


def neighbours(block, axis):
    count = lax.axis_size(axis)
    if count == 1:
        return jnp.zeros_like(block), jnp.zeros_like(block)
    if count == 2:
        other = lax.ppermute(block, axis, [(0, 1), (1, 0)])
        sign = jnp.where(lax.axis_index(axis) == 0, 1.0, -1.0).astype(jnp.float32)
        return other, sign * other
    forward = [(i, i + 1) for i in range(count - 1)]
    below = lax.ppermute(block, axis, forward)
    above = lax.ppermute(block, axis, [(j, i) for i, j in forward])
    return above + below, above - below


def call(kernel, out, scratch, *args):
    return pl.pallas_call(
        kernel,
        out_shape=out,
        scratch_shapes=scratch,
        compiler_params=pltpu.CompilerParams(vmem_limit_bytes=40 * 2**20),
    )(*args)


def on_device(velocity, mode_mask):
    groups = lax.axis_size("pa")
    rank = lax.axis_index("pa")
    depth, kyl, ncols = velocity.shape[1], velocity.shape[3], velocity.shape[4]
    assert depth == 1
    lines = ncols // groups
    half = kyl * groups
    radix = ncols // LANES
    quarter = half // 2
    pieces = HALF // lines
    table = tables(ncols, half, lines)
    f32 = functools.partial(jax.ShapeDtypeStruct, dtype=jnp.float32)
    bf16 = jnp.bfloat16
    speed = velocity[:, 0]
    side, _ = neighbours(speed, "gz")

    def exchange(block):
        return lax.all_to_all(block, "pa", split_axis=0, concat_axis=0, tiled=True)

    def deal(block):
        if pieces == 1:
            return block
        count, rows, _ = block.shape
        block = block.reshape(count, rows, pieces, 2 * lines)
        return jnp.swapaxes(block, 1, 2).reshape(count * pieces, rows, 2 * lines)

    def gather(block):
        if pieces == 1:
            return block
        rows = block.shape[1]
        block = block.reshape(groups // pieces, pieces, rows, 2 * lines)
        return jnp.swapaxes(block, 1, 2).reshape(groups // pieces, rows, LANES)

    def widen(block):
        if lines == HALF:
            return block
        parts = [jnp.pad(p, ((0, 0), (0, 0), (0, HALF - lines))) for p in (block[..., :lines], block[..., lines:])]
        return jnp.concatenate(parts, -1)

    def narrow(block):
        if lines == HALF:
            return block
        return jnp.concatenate([block[..., :lines], block[..., HALF : HALF + lines]], -1)

    sent = call(
        x_forward_kernel,
        f32((2 * radix, 5 * kyl, LANES)),
        [pltpu.VMEM((radix, 5 * kyl, 2 * LANES), jnp.float32)],
        speed,
        table["wave"],
        table["turns"],
        table["forward"],
    )
    received = exchange(deal(sent))
    _, across = neighbours(received[:, : 2 * kyl], "gz")
    sent = call(
        grid_kernel,
        f32((groups, 3 * kyl, LANES)),
        [
            pltpu.VMEM((half, 12 * LANES), bf16),
            pltpu.VMEM((half, 12 * LANES), bf16),
            pltpu.VMEM((quarter, 6 * LANES), bf16),
            pltpu.VMEM((quarter, 6 * LANES), bf16),
        ],
        widen(received),
        widen(0.5 * across),
        table["to_grid"],
        table["from_grid"],
        table["column"],
    )
    received = gather(exchange(narrow(sent)))
    own_modes = rank * kyl + jnp.arange(kyl, dtype=jnp.int32)
    ky = (2.0 * math.pi / (2 * half)) * own_modes.astype(jnp.float32)
    following, partial, w_next = call(
        x_backward_kernel,
        (f32(speed.shape), f32(speed.shape[1:]), f32(speed.shape[1:])),
        [pltpu.VMEM((radix, 3 * kyl, 2 * LANES), jnp.float32)],
        received,
        speed,
        side,
        mode_mask,
        jnp.broadcast_to(ky[:, None], (kyl, LANES)),
        table["wave"],
        table["turns"],
        table["backward"],
    )
    _, across = neighbours(w_next, "gz")
    divergence = partial + 0.5 * across
    return following[:, None], divergence[None]


def solution(mesh):
    placed = (P(None, "gz", None, "pa", None), P("pa", None))
    return jax.shard_map(
        on_device,
        mesh=mesh,
        in_specs=placed,
        out_specs=(P(None, "gz", None, "pa", None), P("gz", None, "pa", None)),
        check_vma=False,
    )
```

```python
import functools
import math

import jax
import jax.numpy as jnp
import ml_dtypes
import numpy as np
from jax import lax
from jax.experimental import pallas as pl
from jax.experimental.pallas import tpu as pltpu
from jax.sharding import PartitionSpec as P

time_step = 0.2
viscosity = 0.25
LANES = 128
HALF = LANES // 2
ROWS = 8


def halves(table):
    high = table.astype(np.float32).astype(ml_dtypes.bfloat16)
    low = (table - high.astype(np.float64)).astype(np.float32).astype(ml_dtypes.bfloat16)
    return np.stack([high, low])


def wheel(rows, cols, period):
    angle = 2.0 * np.pi / period * (np.outer(rows, cols) % period)
    return np.cos(angle), np.sin(angle)


@functools.lru_cache(maxsize=None)
def tables(ncols, half, lines):
    radix = ncols // LANES
    lane = np.arange(LANES)
    scale = 1.0 / math.sqrt(ncols)
    cos, sin = wheel(lane, lane, LANES)
    forward = np.zeros((2 * LANES, 2 * LANES))
    for part in range(LANES // lines):
        x2 = np.arange(part * lines, (part + 1) * lines)
        at = part * 2 * lines
        forward[:LANES, at : at + lines] = cos[:, x2]
        forward[LANES:, at : at + lines] = -sin[:, x2]
        forward[:LANES, at + lines : at + 2 * lines] = sin[:, x2]
        forward[LANES:, at + lines : at + 2 * lines] = cos[:, x2]
    backward = forward.T
    turn_cos, turn_sin = wheel(np.arange(radix), lane, ncols)
    turns = np.concatenate([turn_cos, turn_sin]).astype(np.float32)
    quarter = half // 2
    nrows = 2 * half
    b = np.arange(quarter)
    yscale = 1.0 / math.sqrt(nrows)
    ycos, ysin = wheel(b, b, quarter)
    to_grid = 2.0 * yscale * np.concatenate([ycos, -ysin], 1)
    from_grid = yscale * np.concatenate([ycos, -ysin], 0)
    column = np.zeros((quarter, LANES))
    for y1 in range(1, 4):
        c, s = wheel(b, np.array([y1]), nrows)
        column[:, 2 * y1] = c[:, 0]
        column[:, 2 * y1 + 1] = s[:, 0]
    modes = np.arange(ncols)
    signed = np.where(modes < ncols // 2, modes, modes - ncols).astype(np.float32)
    wave = np.broadcast_to(np.float32(2.0 * math.pi / ncols) * signed, (ROWS, ncols))
    return dict(
        forward=halves(forward * scale),
        backward=halves(backward * scale),
        turns=turns,
        to_grid=halves(to_grid),
        from_grid=halves(from_grid),
        column=column.astype(np.float32),
        wave=np.ascontiguousarray(wave),
    )


def split(value):
    high = value.astype(jnp.bfloat16)
    low = (value - high.astype(jnp.float32)).astype(jnp.bfloat16)
    return high, low


def product(a_high, a_low, b_high, b_low):
    dot = functools.partial(jnp.dot, preferred_element_type=jnp.float32)
    return dot(a_high, b_low) + dot(a_low, b_high) + dot(a_high, b_high)


def butterfly(terms, sign):
    count = len(terms)
    if count == 1:
        return terms
    even = butterfly(terms[0::2], sign)
    odd = butterfly(terms[1::2], sign)
    first, second = [], []
    for k in range(count // 2):
        real, imag = odd[k]
        if k == 0:
            pass
        elif 4 * k == count:
            real, imag = -sign * imag, sign * real
        elif 8 * k == count:
            root = math.sqrt(0.5)
            real, imag = root * (real - sign * imag), root * (imag + sign * real)
        elif 8 * k == 3 * count:
            root = math.sqrt(0.5)
            real, imag = -root * (real + sign * imag), root * (sign * real - imag)
        else:
            c = math.cos(2.0 * math.pi * k / count)
            s = sign * math.sin(2.0 * math.pi * k / count)
            real, imag = c * real - s * imag, s * real + c * imag
        first.append((even[k][0] + real, even[k][1] + imag))
        second.append((even[k][0] - real, even[k][1] - imag))
    return first + second


def x_forward_kernel(plan, vel_ref, wave_ref, turn_ref, mat_ref, out_ref, mid_ref):
    kyl, ncols = vel_ref.shape[2:]
    radix = ncols // LANES
    cols = [slice(a * LANES, (a + 1) * LANES) for a in range(radix)]

    def chunk(c, carry):
        base = pl.multiple_of(c * ROWS, ROWS)
        rows = pl.ds(base, ROWS)
        for slot, (field, slope) in enumerate(plan):
            terms = [(vel_ref[field, 0, rows, s], vel_ref[field, 1, rows, s]) for s in cols]
            if slope:
                terms = [(-wave_ref[:, s] * imag, wave_ref[:, s] * real) for s, (real, imag) in zip(cols, terms)]
            at = pl.ds(pl.multiple_of(slot * kyl + base, ROWS), ROWS)
            for x1, (real, imag) in enumerate(butterfly(terms, 1.0)):
                if x1:
                    cos = turn_ref[x1 : x1 + 1, :]
                    sin = turn_ref[radix + x1 : radix + x1 + 1, :]
                    real, imag = real * cos - imag * sin, real * sin + imag * cos
                mid_ref[x1, at, 0:LANES] = real
                mid_ref[x1, at, LANES : 2 * LANES] = imag
        return carry

    lax.fori_loop(0, kyl // ROWS, chunk, 0)
    for x1 in range(radix):
        high, low = split(mid_ref[x1])
        lines = product(high, low, mat_ref[0], mat_ref[1])
        out_ref[2 * x1] = lines[:, :LANES]
        out_ref[2 * x1 + 1] = lines[:, LANES:]


BLOCK = 32


def swap(value):
    return pltpu.roll(value, HALF, 1)


def left_half(rows):
    return lax.broadcasted_iota(jnp.int32, (rows, LANES), 1) < HALF


def fill(quarter, pairs_at, column_ref, high_ref, low_ref):
    def block(c, carry):
        base = pl.multiple_of(c * BLOCK, BLOCK)
        rows = pl.ds(base, BLOCK)
        lower = pl.ds(pl.multiple_of(quarter + base, BLOCK), BLOCK)
        column = lambda k: jnp.broadcast_to(column_ref[rows, k : k + 1], (BLOCK, LANES))
        near, far = pairs_at(c, 0), pairs_at(c, 1)
        count = len(near)
        for pair in range(count):
            a_re, a_im = near[pair]
            b_re, b_im = far[pair]
            sums = (
                (a_re + b_re, a_im + b_im),
                (a_re - b_im, a_im + b_re),
                (a_re - b_re, a_im - b_im),
                (a_re + b_im, a_im - b_re),
            )
            for y1, (real, imag) in enumerate(sums):
                if y1:
                    cos = column(2 * y1)
                    sin = column(2 * y1 + 1)
                    real, imag = real * cos - imag * sin, real * sin + imag * cos
                at = slice((count * y1 + pair) * LANES, (count * y1 + pair + 1) * LANES)
                high_ref[rows, at], low_ref[rows, at] = split(real)
                high_ref[lower, at], low_ref[lower, at] = split(imag)
        return carry

    lax.fori_loop(0, quarter // BLOCK, block, 0)


def reader(groups, kyl, quarter):
    each = BLOCK // kyl
    left = left_half(BLOCK)

    def load(ref, f, c, far):
        sources = pl.ds(c * each + far * (groups // 2), each)
        return ref[sources, f * kyl : (f + 1) * kyl, :].reshape(BLOCK, LANES)

    def modes(c, far):
        index = c * BLOCK + far * quarter + lax.broadcasted_iota(jnp.int32, (BLOCK, LANES), 0)
        ky = index.astype(jnp.float32) * (2.0 * math.pi / (4 * quarter))
        return jnp.where(index == 0, 0.5, 1.0), jnp.where(left, -ky, ky)

    def paired(one, two, weight):
        one = one * weight
        two = two * weight
        return jnp.where(left, one, swap(two)), jnp.where(left, swap(one), two)

    return load, modes, paired


def speed_kernel(uv_ref, to_ref, column_ref, grid_ref, high_ref, low_ref):
    groups, kyl = uv_ref.shape[0], uv_ref.shape[1] // 2
    quarter = groups * kyl // 2
    load, modes, paired = reader(groups, kyl, quarter)

    def pairs_at(c, far):
        weight, _ = modes(c, far)
        return [paired(load(uv_ref, 0, c, far), load(uv_ref, 1, c, far), weight)]

    fill(quarter, pairs_at, column_ref, high_ref, low_ref)
    grid_ref[...] = product(to_ref[0], to_ref[1], high_ref[...], low_ref[...])


def cross_kernel(uv_ref, wall_ref, rest_ref, grid_ref, to_ref, from_ref, column_ref, out_ref, yx_high, yx_low, high_ref, low_ref, z_high, z_low):
    groups, kyl = uv_ref.shape[0], uv_ref.shape[1] // 2
    quarter = groups * kyl // 2
    load, modes, paired = reader(groups, kyl, quarter)

    def pairs_at(c, far):
        weight, ky = modes(c, far)
        u = load(uv_ref, 0, c, far)
        du_dz, dv_dz = load(wall_ref, 0, c, far), load(wall_ref, 1, c, far)
        w, dw, dv = [load(rest_ref, f, c, far) for f in range(3)]
        omega_x = ky * swap(w) - dv_dz
        omega_y = du_dz - dw
        omega_z = dv - ky * swap(u)
        return [paired(omega_x, omega_y, weight), paired(w, omega_z, weight)]

    fill(quarter, pairs_at, column_ref, high_ref, low_ref)
    wide = left_half(quarter)
    kept = None
    for y1 in range(4):
        at = slice(2 * y1 * LANES, 2 * (y1 + 1) * LANES)
        grid = product(to_ref[0], to_ref[1], high_ref[:, at], low_ref[:, at])
        slot = slice(y1 * LANES, (y1 + 1) * LANES)
        uv = grid_ref[:, slot]
        xy = grid[:, :LANES]
        wz = grid[:, LANES:]
        zw = swap(wz)
        h_yx = jnp.where(wide, wz, zw) * xy - jnp.where(wide, zw, wz) * uv
        spin = uv * swap(xy)
        h_z = spin - swap(spin)
        yx_high[:, slot], yx_low[:, slot] = split(h_yx)
        if y1 % 2 == 0:
            kept = h_z
        else:
            slot = slice(y1 // 2 * LANES, (y1 // 2 + 1) * LANES)
            z_high[:, slot], z_low[:, slot] = split(jnp.where(wide, kept, -h_z))
    freq = product(from_ref[0], from_ref[1], z_high[...], z_low[...])
    turn = turns_of(column_ref, quarter)
    one = jnp.ones((quarter, LANES), jnp.float32)
    zero = jnp.zeros((quarter, LANES), jnp.float32)
    z01 = piece(freq, quarter, 0, jnp.where(wide, one, turn[1][0]), jnp.where(wide, zero, turn[1][1]))
    z23 = piece(freq, quarter, 1, jnp.where(wide, turn[2][0], turn[3][0]), jnp.where(wide, turn[2][1], turn[3][1]))
    v_re, v_im = z01[0] + z23[0], z01[1] + z23[1]
    d_re, d_im = z01[0] - z23[0], z01[1] - z23[1]
    store(out_ref, kyl, 0, 0, jnp.where(wide, v_re + swap(v_re), v_im + swap(v_im)))
    store(out_ref, kyl, 1, 0, jnp.where(wide, d_re + swap(d_im), swap(d_im) - d_re))


def turns_of(column_ref, quarter):
    column = lambda k: jnp.broadcast_to(column_ref[:, k : k + 1], (quarter, LANES))
    return [(None, None)] + [(column(2 * y1), column(2 * y1 + 1)) for y1 in range(1, 4)]


def piece(freq, quarter, slot, cos, sin):
    real = freq[:quarter, slot * LANES : (slot + 1) * LANES]
    imag = freq[quarter:, slot * LANES : (slot + 1) * LANES]
    if cos is None:
        return real, imag
    return real * cos + imag * sin, imag * cos - real * sin


def store(out_ref, kyl, far, field, value):
    gap = out_ref.shape[0] // 2
    for s in range(gap):
        out_ref[far * gap + s, field * kyl : (field + 1) * kyl, :] = value[s * kyl : (s + 1) * kyl]


def return_kernel(yx_high, yx_low, from_ref, column_ref, out_ref):
    quarter = column_ref.shape[0]
    kyl = out_ref.shape[1] // 2
    wide = left_half(quarter)
    freq = product(from_ref[0], from_ref[1], yx_high[...], yx_low[...])
    turn = turns_of(column_ref, quarter)
    q0, q1, q2, q3 = [piece(freq, quarter, y1, *turn[y1]) for y1 in range(4)]
    near_re = q0[0] + q1[0] + q2[0] + q3[0]
    near_im = q0[1] + q1[1] + q2[1] + q3[1]
    far_re = q0[0] + q1[1] - q2[0] - q3[1]
    far_im = q0[1] - q1[0] - q2[1] + q3[0]
    for far, real, imag in ((0, near_re, near_im), (1, far_re, far_im)):
        store(out_ref, kyl, far, 0, -jnp.where(wide, swap(real), imag))
        store(out_ref, kyl, far, 1, jnp.where(wide, real, swap(imag)))


def to_modes(recv_ref, turn_ref, mat_ref, mid_ref):
    radix = mid_ref.shape[0]
    for x1 in range(radix):
        high, low = split(jnp.concatenate([recv_ref[2 * x1], recv_ref[2 * x1 + 1]], axis=1))
        freq = product(high, low, mat_ref[0], mat_ref[1])
        real = freq[:, :LANES]
        imag = freq[:, LANES:]
        if x1:
            cos = turn_ref[x1 : x1 + 1, :]
            sin = turn_ref[radix + x1 : radix + x1 + 1, :]
            real, imag = real * cos + imag * sin, imag * cos - real * sin
        mid_ref[x1, :, 0:LANES] = real
        mid_ref[x1, :, LANES : 2 * LANES] = imag


def advance(field, slot, kyl, base, vel_ref, side_ref, mask_ref, ky_ref, wave_ref, mid_ref):
    radix = mid_ref.shape[0]
    rows = pl.ds(base, ROWS)
    ky = ky_ref[rows, :]
    at = pl.ds(pl.multiple_of(slot * kyl + base, ROWS), ROWS)
    terms = [(mid_ref[x1, at, 0:LANES], mid_ref[x1, at, LANES : 2 * LANES]) for x1 in range(radix)]
    for a, pair in enumerate(butterfly(terms, -1.0)):
        cols = slice(a * LANES, (a + 1) * LANES)
        kx = wave_ref[:, cols]
        keep = mask_ref[rows, cols] != 0
        decay = viscosity * (2.0 + kx * kx + ky * ky)
        fresh = []
        for part in range(2):
            speed = vel_ref[field, part, rows, cols]
            change = jnp.where(keep, pair[part], 0.0)
            change = change + viscosity * side_ref[field, part, rows, cols] - decay * speed
            fresh.append(speed + time_step * change)
        yield cols, kx, ky, fresh[0], fresh[1]


def wall_kernel(recv_ref, vel_ref, side_ref, mask_ref, ky_ref, wave_ref, turn_ref, mat_ref, w_ref, mid_ref):
    kyl = vel_ref.shape[2]
    to_modes(recv_ref, turn_ref, mat_ref, mid_ref)

    def chunk(c, carry):
        base = pl.multiple_of(c * ROWS, ROWS)
        rows = pl.ds(base, ROWS)
        for cols, _, _, real, imag in advance(2, 0, kyl, base, vel_ref, side_ref, mask_ref, ky_ref, wave_ref, mid_ref):
            w_ref[0, rows, cols] = real
            w_ref[1, rows, cols] = imag
        return carry

    lax.fori_loop(0, kyl // ROWS, chunk, 0)


def final_kernel(recv_ref, vel_ref, side_ref, mask_ref, ky_ref, wave_ref, turn_ref, mat_ref, w_ref, across_ref, sign_ref, next_ref, div_ref, mid_ref):
    kyl = vel_ref.shape[2]
    to_modes(recv_ref, turn_ref, mat_ref, mid_ref)
    next_ref[2] = w_ref[...]
    sign = sign_ref[0:1, :]

    def chunk(c, carry):
        base = pl.multiple_of(c * ROWS, ROWS)
        rows = pl.ds(base, ROWS)
        shared = (kyl, base, vel_ref, side_ref, mask_ref, ky_ref, wave_ref, mid_ref)
        for one, two in zip(advance(0, 0, *shared), advance(1, 1, *shared)):
            cols, kx, ky, u_re, u_im = one
            v_re, v_im = two[3:]
            next_ref[0, 0, rows, cols] = u_re
            next_ref[0, 1, rows, cols] = u_im
            next_ref[1, 0, rows, cols] = v_re
            next_ref[1, 1, rows, cols] = v_im
            div_ref[0, rows, cols] = sign * across_ref[0, rows, cols] - kx * u_im - ky * v_im
            div_ref[1, rows, cols] = sign * across_ref[1, rows, cols] + kx * u_re + ky * v_re
        return carry

    lax.fori_loop(0, kyl // ROWS, chunk, 0)


def neighbours(block, axis):
    count = lax.axis_size(axis)
    if count == 1:
        return jnp.zeros_like(block), jnp.zeros_like(block), jnp.float32(1.0)
    if count == 2:
        other = lax.ppermute(block, axis, [(0, 1), (1, 0)])
        return other, other, jnp.where(lax.axis_index(axis) == 0, 1.0, -1.0).astype(jnp.float32)
    forward = [(i, i + 1) for i in range(count - 1)]
    below = lax.ppermute(block, axis, forward)
    above = lax.ppermute(block, axis, [(j, i) for i, j in forward])
    return above + below, above - below, jnp.float32(1.0)


def call(kernel, out, scratch, *args):
    return pl.pallas_call(
        kernel,
        out_shape=out,
        scratch_shapes=scratch,
        compiler_params=pltpu.CompilerParams(vmem_limit_bytes=40 * 2**20),
    )(*args)


def on_device(velocity, mode_mask):
    groups = lax.axis_size("pa")
    rank = lax.axis_index("pa")
    depth, kyl, ncols = velocity.shape[1], velocity.shape[3], velocity.shape[4]
    assert depth == 1
    lines = ncols // groups
    half = kyl * groups
    radix = ncols // LANES
    quarter = half // 2
    pieces = HALF // lines
    table = tables(ncols, half, lines)
    f32 = functools.partial(jax.ShapeDtypeStruct, dtype=jnp.float32)
    bf16 = jnp.bfloat16
    speed = velocity[:, 0]
    side, _, _ = neighbours(speed, "gz")

    def exchange(block):
        return lax.all_to_all(block, "pa", split_axis=0, concat_axis=0, tiled=True)

    def deal(block):
        if pieces == 1:
            return block
        count, rows, _ = block.shape
        block = block.reshape(count, rows, pieces, 2 * lines)
        return jnp.swapaxes(block, 1, 2).reshape(count * pieces, rows, 2 * lines)

    def gather(block):
        if pieces == 1:
            return block
        rows = block.shape[1]
        block = block.reshape(groups // pieces, pieces, rows, 2 * lines)
        return jnp.swapaxes(block, 1, 2).reshape(groups // pieces, rows, LANES)

    def widen(block):
        if lines == HALF:
            return block
        parts = [jnp.pad(p, ((0, 0), (0, 0), (0, HALF - lines))) for p in (block[..., :lines], block[..., lines:])]
        return jnp.concatenate(parts, -1)

    def narrow(block):
        if lines == HALF:
            return block
        return jnp.concatenate([block[..., :lines], block[..., HALF : HALF + lines]], -1)

    x_tables = (table["wave"], table["turns"], table["forward"])

    def x_forward(*plan):
        count = len(plan) * kyl
        scratch = [pltpu.VMEM((radix, count, 2 * LANES), jnp.float32)]
        kernel = functools.partial(x_forward_kernel, plan)
        return exchange(deal(call(kernel, f32((2 * radix, count, LANES)), scratch, speed, *x_tables)))

    uv = x_forward((0, False), (1, False))
    rest = x_forward((2, False), (2, True), (1, True))
    _, across, sign = neighbours(uv, "gz")
    uv = widen(uv)
    pair = lambda count: [pltpu.VMEM((half, 4 * count * LANES), bf16)] * 2
    grid_uv = call(
        speed_kernel, f32((quarter, 4 * LANES)), pair(1), uv, table["to_grid"], table["column"]
    )
    packed = jax.ShapeDtypeStruct((quarter, 4 * LANES), bf16)
    sent_z, yx_high, yx_low = call(
        cross_kernel,
        (f32((groups, kyl, LANES)), packed, packed),
        pair(2) + [pltpu.VMEM((quarter, 2 * LANES), bf16)] * 2,
        uv,
        widen(across * (0.5 * sign)),
        widen(rest),
        grid_uv,
        table["to_grid"],
        table["from_grid"],
        table["column"],
    )
    z_lines = gather(exchange(narrow(sent_z)))
    sent_xy = call(
        return_kernel, f32((groups, 2 * kyl, LANES)), [], yx_high, yx_low, table["from_grid"], table["column"]
    )
    xy_lines = gather(exchange(narrow(sent_xy)))
    own_modes = rank * kyl + jnp.arange(kyl, dtype=jnp.int32)
    ky = (2.0 * math.pi / (2 * half)) * own_modes.astype(jnp.float32)
    ky = jnp.broadcast_to(ky[:, None], (kyl, LANES))
    shared = (speed, side, mode_mask, ky, table["wave"], table["turns"], table["backward"])
    mid = lambda count: [pltpu.VMEM((radix, count * kyl, 2 * LANES), jnp.float32)]
    w_next = call(wall_kernel, f32(speed.shape[1:]), mid(1), z_lines, *shared)
    _, across, sign = neighbours(w_next, "gz")
    following, divergence = call(
        final_kernel,
        (f32(speed.shape), f32(speed.shape[1:])),
        mid(2),
        xy_lines,
        *shared,
        w_next,
        across,
        jnp.broadcast_to(0.5 * sign, (ROWS, LANES)),
    )
    return following[:, None], divergence[None]


def solution(mesh):
    placed = (P(None, "gz", None, "pa", None), P("pa", None))
    return jax.shard_map(
        on_device,
        mesh=mesh,
        in_specs=placed,
        out_specs=(P(None, "gz", None, "pa", None), P("gz", None, "pa", None)),
        check_vma=False,
    )
```

```python
import functools
import math

import jax
import jax.numpy as jnp
import ml_dtypes
import numpy as np
from jax import lax
from jax.experimental import pallas as pl
from jax.experimental.pallas import tpu as pltpu
from jax.sharding import PartitionSpec as P

time_step = 0.2
viscosity = 0.25
LANES = 128
HALF = LANES // 2
ROWS = 8
MOST = 16


def halves(table):
    high = table.astype(np.float32).astype(ml_dtypes.bfloat16)
    low = (table - high.astype(np.float64)).astype(np.float32).astype(ml_dtypes.bfloat16)
    return np.stack([high, low])


def wheel(rows, cols, period):
    angle = 2.0 * np.pi / period * (np.outer(rows, cols) % period)
    return np.cos(angle), np.sin(angle)


@functools.lru_cache(maxsize=None)
def tables(ncols, half, lines):
    radix = ncols // LANES
    lane = np.arange(LANES)
    scale = 1.0 / math.sqrt(ncols)
    cos, sin = wheel(lane, lane, LANES)
    forward = np.zeros((2 * LANES, 2 * LANES))
    for part in range(LANES // lines):
        x2 = np.arange(part * lines, (part + 1) * lines)
        at = part * 2 * lines
        forward[:LANES, at : at + lines] = cos[:, x2]
        forward[LANES:, at : at + lines] = -sin[:, x2]
        forward[:LANES, at + lines : at + 2 * lines] = sin[:, x2]
        forward[LANES:, at + lines : at + 2 * lines] = cos[:, x2]
    backward = forward.T
    turn_cos, turn_sin = wheel(np.arange(radix), lane, ncols)
    turns = np.concatenate([turn_cos, turn_sin]).astype(np.float32)
    quarter = half // 2
    nrows = 2 * half
    b = np.arange(quarter)
    yscale = 1.0 / math.sqrt(nrows)
    ycos, ysin = wheel(b, b, quarter)
    to_grid = 2.0 * yscale * np.concatenate([ycos, -ysin], 1)
    from_grid = yscale * np.concatenate([ycos, -ysin], 0)
    column = np.zeros((quarter, LANES))
    for y1 in range(1, 4):
        c, s = wheel(b, np.array([y1]), nrows)
        column[:, 2 * y1] = c[:, 0]
        column[:, 2 * y1 + 1] = s[:, 0]
    modes = np.arange(ncols)
    signed = np.where(modes < ncols // 2, modes, modes - ncols).astype(np.float32)
    wave = np.broadcast_to(np.float32(2.0 * math.pi / ncols) * signed, (ROWS, ncols))
    return dict(
        forward=halves(forward * scale),
        backward=halves(backward * scale),
        turns=turns,
        to_grid=halves(to_grid),
        from_grid=halves(from_grid),
        column=column.astype(np.float32),
        wave=np.ascontiguousarray(wave),
    )


def split(value):
    high = value.astype(jnp.bfloat16)
    low = (value - high.astype(jnp.float32)).astype(jnp.bfloat16)
    return high, low


def product(a_high, a_low, b_high, b_low):
    dot = functools.partial(jnp.dot, preferred_element_type=jnp.float32)
    return dot(a_high, b_low) + dot(a_low, b_high) + dot(a_high, b_high)


def butterfly(terms, sign):
    count = len(terms)
    if count == 1:
        return terms
    even = butterfly(terms[0::2], sign)
    odd = butterfly(terms[1::2], sign)
    first, second = [], []
    for k in range(count // 2):
        real, imag = odd[k]
        if k == 0:
            pass
        elif 4 * k == count:
            real, imag = -sign * imag, sign * real
        elif 8 * k == count:
            root = math.sqrt(0.5)
            real, imag = root * (real - sign * imag), root * (imag + sign * real)
        elif 8 * k == 3 * count:
            root = math.sqrt(0.5)
            real, imag = -root * (real + sign * imag), root * (sign * real - imag)
        else:
            c = math.cos(2.0 * math.pi * k / count)
            s = sign * math.sin(2.0 * math.pi * k / count)
            real, imag = c * real - s * imag, s * real + c * imag
        first.append((even[k][0] + real, even[k][1] + imag))
        second.append((even[k][0] - real, even[k][1] - imag))
    return first + second


def scatter(order_ref, all_ref, out_refs):
    if len(out_refs) == 1:
        out_refs[0][...] = all_ref[...]
        return
    for k, out_ref in enumerate(out_refs):
        out_ref[...] = all_ref[order_ref[k]]


def collect(order_ref, in_refs, all_ref):
    if len(in_refs) == 1:
        all_ref[...] = in_refs[0][...]
        return
    for k, in_ref in enumerate(in_refs):
        all_ref[order_ref[k]] = in_ref[...]


def x_forward_kernel(order_ref, vel_hbm, wave_hbm, turn_hbm, mat_hbm, *rest):
    out_refs = rest[:-7]
    vel_ref, wave_ref, turn_ref, mat_ref, mid_ref, all_ref, sems = rest[-7:]
    kyl, ncols = vel_ref.shape[2:]
    radix = ncols // LANES
    moves = ((vel_hbm, vel_ref), (wave_hbm, wave_ref), (turn_hbm, turn_ref), (mat_hbm, mat_ref))
    copies = [pltpu.make_async_copy(src, dst, sems.at[i]) for i, (src, dst) in enumerate(moves)]
    for copy in copies:
        copy.start()
    for copy in copies:
        copy.wait()

    def chunk(c, carry):
        base = pl.multiple_of(c * ROWS, ROWS)
        rows = pl.ds(base, ROWS)

        def emit(field, terms):
            for x1, (real, imag) in enumerate(butterfly(terms, 1.0)):
                if x1:
                    cos = turn_ref[x1 : x1 + 1, :]
                    sin = turn_ref[radix + x1 : radix + x1 + 1, :]
                    real, imag = real * cos - imag * sin, real * sin + imag * cos
                at = pl.ds(pl.multiple_of(field * kyl + base, ROWS), ROWS)
                mid_ref[x1, at, 0:LANES] = real
                mid_ref[x1, at, LANES : 2 * LANES] = imag

        def load(field):
            cols = [slice(a * LANES, (a + 1) * LANES) for a in range(radix)]
            return [(vel_ref[field, 0, rows, s], vel_ref[field, 1, rows, s]) for s in cols]

        def slope(terms):
            waves = [wave_ref[:, a * LANES : (a + 1) * LANES] for a in range(radix)]
            return [(-k * imag, k * real) for k, (real, imag) in zip(waves, terms)]

        emit(0, load(0))
        emit(1, load(1))
        emit(2, load(2))
        emit(3, slope(load(2)))
        emit(4, slope(load(1)))
        return carry

    lax.fori_loop(0, kyl // ROWS, chunk, 0)
    for x1 in range(radix):
        high, low = split(mid_ref[x1])
        lines = product(high, low, mat_ref[0], mat_ref[1])
        all_ref[2 * x1] = lines[:, :LANES]
        all_ref[2 * x1 + 1] = lines[:, LANES:]
    scatter(order_ref, all_ref, out_refs)


def grid_kernel(count, outs, order_ref, *rest):
    wall_in, to_ref, from_ref, column_ref = rest[count : count + 4]
    out_refs = rest[count + 4 : count + 4 + outs]
    high_ref, low_ref, back_high, back_low, recv_ref, out_ref, wall_ref = rest[count + 4 + outs :]
    collect(order_ref, rest[:count], recv_ref)
    collect(order_ref, [wall_in.at[k] for k in range(count)] if count > 1 else [wall_in], wall_ref)
    groups = recv_ref.shape[0]
    kyl = recv_ref.shape[1] // 5
    quarter = groups * kyl // 2
    block = 32
    each = block // kyl
    gap = groups // 2
    ky_step = 2.0 * math.pi / (4 * quarter)
    left = lax.broadcasted_iota(jnp.int32, (block, LANES), 1) < HALF
    swap = lambda value: pltpu.roll(value, HALF, 1)

    def fields(first, row):
        sources = pl.ds(first, each)
        load = lambda ref, f: ref[sources, f * kyl : (f + 1) * kyl, :].reshape(block, LANES)

        index = row + lax.broadcasted_iota(jnp.int32, (block, LANES), 0)
        ky = index.astype(jnp.float32) * ky_step
        weight = jnp.where(index == 0, 0.5, 1.0)
        ky_signed = jnp.where(left, -ky, ky)
        u, v, w, dw, dv = [load(recv_ref, f) for f in range(5)]
        du_dz, dv_dz = load(wall_ref, 0), load(wall_ref, 1)
        omega_x = ky_signed * swap(w) - dv_dz
        omega_y = du_dz - dw
        omega_z = dv - ky_signed * swap(u)
        result = []
        for one, two in ((u, v), (omega_x, omega_y), (w, omega_z)):
            one = one * weight
            two = two * weight
            result.append((jnp.where(left, one, swap(two)), jnp.where(left, swap(one), two)))
        return result

    def column(rows, k):
        return jnp.broadcast_to(column_ref[rows, k : k + 1], (block, LANES))

    def load_block(c, carry):
        base = pl.multiple_of(c * block, block)
        rows = pl.ds(base, block)
        near = fields(c * each, base)
        far = fields(c * each + gap, base + quarter)
        for pair in range(3):
            a_re, a_im = near[pair]
            b_re, b_im = far[pair]
            sums = (
                (a_re + b_re, a_im + b_im),
                (a_re - b_im, a_im + b_re),
                (a_re - b_re, a_im - b_im),
                (a_re + b_im, a_im - b_re),
            )
            for y1, (real, imag) in enumerate(sums):
                if y1:
                    cos = column(rows, 2 * y1)
                    sin = column(rows, 2 * y1 + 1)
                    real, imag = real * cos - imag * sin, real * sin + imag * cos
                at = slice((3 * y1 + pair) * LANES, (3 * y1 + pair + 1) * LANES)
                lower = pl.ds(pl.multiple_of(quarter + base, block), block)
                high_ref[rows, at], low_ref[rows, at] = split(real)
                high_ref[lower, at], low_ref[lower, at] = split(imag)
        return carry

    lax.fori_loop(0, quarter // block, load_block, 0)

    wide = lax.broadcasted_iota(jnp.int32, (quarter, LANES), 1) < HALF
    kept = None
    for y1 in range(4):
        at = slice(3 * y1 * LANES, 3 * (y1 + 1) * LANES)
        grid = product(to_ref[0], to_ref[1], high_ref[:, at], low_ref[:, at])
        uv = grid[:, :LANES]
        xy = grid[:, LANES : 2 * LANES]
        wz = grid[:, 2 * LANES :]
        zw = swap(wz)
        h_yx = jnp.where(wide, wz, zw) * xy - jnp.where(wide, zw, wz) * uv
        spin = uv * swap(xy)
        h_z = spin - swap(spin)
        slot = slice(y1 * LANES, (y1 + 1) * LANES)
        back_high[:, slot], back_low[:, slot] = split(h_yx)
        if y1 % 2 == 0:
            kept = h_z
        else:
            slot = slice((4 + y1 // 2) * LANES, (5 + y1 // 2) * LANES)
            back_high[:, slot], back_low[:, slot] = split(jnp.where(wide, kept, -h_z))

    freq = product(from_ref[0], from_ref[1], back_high[...], back_low[...])

    column_all = lambda k: jnp.broadcast_to(column_ref[:, k : k + 1], (quarter, LANES))

    def piece(slot, cos, sin):
        real = freq[:quarter, slot * LANES : (slot + 1) * LANES]
        imag = freq[quarter:, slot * LANES : (slot + 1) * LANES]
        if cos is None:
            return real, imag
        return real * cos + imag * sin, imag * cos - real * sin

    turn = [(None, None)] + [(column_all(2 * y1), column_all(2 * y1 + 1)) for y1 in range(1, 4)]
    one = jnp.ones((quarter, LANES), jnp.float32)
    zero = jnp.zeros((quarter, LANES), jnp.float32)
    q0, q1, q2, q3 = [piece(y1, *turn[y1]) for y1 in range(4)]
    z01 = piece(4, jnp.where(wide, one, turn[1][0]), jnp.where(wide, zero, turn[1][1]))
    z23 = piece(5, jnp.where(wide, turn[2][0], turn[3][0]), jnp.where(wide, turn[2][1], turn[3][1]))
    near_re = q0[0] + q1[0] + q2[0] + q3[0]
    near_im = q0[1] + q1[1] + q2[1] + q3[1]
    far_re = q0[0] + q1[1] - q2[0] - q3[1]
    far_im = q0[1] - q1[0] - q2[1] + q3[0]
    v_re, v_im = z01[0] + z23[0], z01[1] + z23[1]
    z_near = jnp.where(wide, v_re + swap(v_re), v_im + swap(v_im))
    d_re, d_im = z01[0] - z23[0], z01[1] - z23[1]
    z_far = jnp.where(wide, d_re + swap(d_im), swap(d_im) - d_re)

    def store(first, field, value):
        for s in range(gap):
            out_ref[first + s, field * kyl : (field + 1) * kyl, :] = value[s * kyl : (s + 1) * kyl]

    for first, real, imag, h_z in ((0, near_re, near_im, z_near), (gap, far_re, far_im, z_far)):
        store(first, 0, -jnp.where(wide, swap(real), imag))
        store(first, 1, jnp.where(wide, real, swap(imag)))
        store(first, 2, h_z)
    scatter(order_ref, out_ref, out_refs)


def x_backward_kernel(count, order_ref, *rest):
    vel_ref, side_ref, mask_ref, ky_ref, wave_ref, turn_ref, mat_ref, next_ref, div_ref, w_ref, mid_ref, recv_ref = rest[count:]
    collect(order_ref, rest[:count], recv_ref)
    kyl, ncols = vel_ref.shape[2:]
    radix = ncols // LANES
    for x1 in range(radix):
        high, low = split(jnp.concatenate([recv_ref[2 * x1], recv_ref[2 * x1 + 1]], axis=1))
        freq = product(high, low, mat_ref[0], mat_ref[1])
        real = freq[:, :LANES]
        imag = freq[:, LANES:]
        if x1:
            cos = turn_ref[x1 : x1 + 1, :]
            sin = turn_ref[radix + x1 : radix + x1 + 1, :]
            real, imag = real * cos + imag * sin, imag * cos - real * sin
        mid_ref[x1, :, 0:LANES] = real
        mid_ref[x1, :, LANES : 2 * LANES] = imag

    def chunk(c, carry):
        base = pl.multiple_of(c * ROWS, ROWS)
        rows = pl.ds(base, ROWS)
        ky = ky_ref[rows, :]
        for field in range(3):
            at = pl.ds(pl.multiple_of(field * kyl + base, ROWS), ROWS)
            terms = [(mid_ref[x1, at, 0:LANES], mid_ref[x1, at, LANES : 2 * LANES]) for x1 in range(radix)]
            for a, pair in enumerate(butterfly(terms, -1.0)):
                cols = slice(a * LANES, (a + 1) * LANES)
                kx = wave_ref[:, cols]
                keep = mask_ref[rows, cols] != 0
                decay = viscosity * (2.0 + kx * kx + ky * ky)
                fresh = []
                for part in range(2):
                    speed = vel_ref[field, part, rows, cols]
                    change = jnp.where(keep, pair[part], 0.0)
                    change = change + viscosity * side_ref[field, part, rows, cols] - decay * speed
                    fresh.append(speed + time_step * change)
                    next_ref[field, part, rows, cols] = fresh[part]
                if field == 0:
                    div_ref[0, rows, cols] = -kx * fresh[1]
                    div_ref[1, rows, cols] = kx * fresh[0]
                elif field == 1:
                    div_ref[0, rows, cols] = div_ref[0, rows, cols] - ky * fresh[1]
                    div_ref[1, rows, cols] = div_ref[1, rows, cols] + ky * fresh[0]
                else:
                    w_ref[0, rows, cols] = fresh[0]
                    w_ref[1, rows, cols] = fresh[1]
        return carry

    lax.fori_loop(0, kyl // ROWS, chunk, 0)


def neighbours(block, axis):
    count = lax.axis_size(axis)
    if count == 1:
        return jnp.zeros_like(block), jnp.zeros_like(block)
    if count == 2:
        other = lax.ppermute(block, axis, [(0, 1), (1, 0)])
        sign = jnp.where(lax.axis_index(axis) == 0, 1.0, -1.0).astype(jnp.float32)
        return other, sign * other
    forward = [(i, i + 1) for i in range(count - 1)]
    below = lax.ppermute(block, axis, forward)
    above = lax.ppermute(block, axis, [(j, i) for i, j in forward])
    return above + below, above - below


def call(kernel, out, scratch, *args, hbm=()):
    whole = pl.BlockSpec(memory_space=pltpu.VMEM)
    spec = {0: pl.BlockSpec(memory_space=pltpu.SMEM)}
    spec.update({i: pl.BlockSpec(memory_space=pltpu.HBM) for i in hbm})
    return pl.pallas_call(
        kernel,
        in_specs=[spec.get(i, whole) for i in range(len(args))],
        out_shape=out,
        scratch_shapes=scratch,
        compiler_params=pltpu.CompilerParams(vmem_limit_bytes=40 * 2**20),
    )(*args)


def on_device(velocity, mode_mask):
    groups = lax.axis_size("pa")
    rank = lax.axis_index("pa")
    depth, kyl, ncols = velocity.shape[1], velocity.shape[3], velocity.shape[4]
    assert depth == 1
    lines = ncols // groups
    half = kyl * groups
    radix = ncols // LANES
    quarter = half // 2
    pieces = HALF // lines
    table = tables(ncols, half, lines)
    f32 = functools.partial(jax.ShapeDtypeStruct, dtype=jnp.float32)
    bf16 = jnp.bfloat16
    speed = velocity[:, 0]
    side, _ = neighbours(speed, "gz")

    direct = pieces == 1 and lines == HALF and groups & (groups - 1) == 0 and groups <= MOST
    order = jnp.bitwise_xor(rank, jnp.arange(groups, dtype=jnp.int32)).astype(jnp.int32)

    def exchange(blocks):
        if not direct:
            return [lax.all_to_all(blocks[0], "pa", split_axis=0, concat_axis=0, tiled=True)]
        moved = [blocks[0]]
        for k in range(1, groups):
            moved.append(lax.ppermute(blocks[k], "pa", [(i, i ^ k) for i in range(groups)]))
        return moved

    def pieces_of(rows, count):
        if direct:
            return [f32((rows, LANES)) for _ in range(count)]
        return [f32((count, rows, LANES))]

    def deal(block):
        if pieces == 1:
            return block
        count, rows, _ = block.shape
        block = block.reshape(count, rows, pieces, 2 * lines)
        return jnp.swapaxes(block, 1, 2).reshape(count * pieces, rows, 2 * lines)

    def gather(block):
        if pieces == 1:
            return block
        rows = block.shape[1]
        block = block.reshape(groups // pieces, pieces, rows, 2 * lines)
        return jnp.swapaxes(block, 1, 2).reshape(groups // pieces, rows, LANES)

    def widen(block):
        if lines == HALF:
            return block
        parts = [jnp.pad(p, ((0, 0), (0, 0), (0, HALF - lines))) for p in (block[..., :lines], block[..., lines:])]
        return jnp.concatenate(parts, -1)

    def narrow(block):
        if lines == HALF:
            return block
        return jnp.concatenate([block[..., :lines], block[..., HALF : HALF + lines]], -1)

    here = lambda array: pltpu.VMEM(array.shape, array.dtype)
    count = groups if direct else 1
    sent = call(
        x_forward_kernel,
        pieces_of(5 * kyl, 2 * radix),
        [
            pltpu.VMEM(speed.shape, jnp.float32),
            here(table["wave"]),
            here(table["turns"]),
            here(table["forward"]),
            pltpu.VMEM((radix, 5 * kyl, 2 * LANES), jnp.float32),
            pltpu.VMEM((2 * radix, 5 * kyl, LANES), jnp.float32),
            pltpu.SemaphoreType.DMA((4,)),
        ],
        order,
        speed,
        table["wave"],
        table["turns"],
        table["forward"],
        hbm=(1, 2, 3, 4),
    )
    received = exchange([sent[0] if direct else deal(sent[0])] + list(sent[1:]))
    if direct:
        stacked = jnp.stack([block[: 2 * kyl] for block in received])
    else:
        stacked = received[0][:, : 2 * kyl]
    _, across = neighbours(stacked, "gz")
    sent = call(
        functools.partial(grid_kernel, count, count),
        pieces_of(3 * kyl, groups),
        [
            pltpu.VMEM((half, 12 * LANES), bf16),
            pltpu.VMEM((half, 12 * LANES), bf16),
            pltpu.VMEM((quarter, 6 * LANES), bf16),
            pltpu.VMEM((quarter, 6 * LANES), bf16),
            pltpu.VMEM((groups, 5 * kyl, LANES), jnp.float32),
            pltpu.VMEM((groups, 3 * kyl, LANES), jnp.float32),
            pltpu.VMEM((groups, 2 * kyl, LANES), jnp.float32),
        ],
        order,
        *[widen(block) for block in received],
        widen(0.5 * across),
        table["to_grid"],
        table["from_grid"],
        table["column"],
    )
    received = exchange([narrow(block) for block in sent])
    if not direct:
        received = [gather(received[0])]
    own_modes = rank * kyl + jnp.arange(kyl, dtype=jnp.int32)
    ky = (2.0 * math.pi / (2 * half)) * own_modes.astype(jnp.float32)
    following, partial, w_next = call(
        functools.partial(x_backward_kernel, count),
        (f32(speed.shape), f32(speed.shape[1:]), f32(speed.shape[1:])),
        [
            pltpu.VMEM((radix, 3 * kyl, 2 * LANES), jnp.float32),
            pltpu.VMEM((2 * radix, 3 * kyl, LANES), jnp.float32),
        ],
        order,
        *received,
        speed,
        side,
        mode_mask,
        jnp.broadcast_to(ky[:, None], (kyl, LANES)),
        table["wave"],
        table["turns"],
        table["backward"],
    )
    _, across = neighbours(w_next, "gz")
    divergence = partial + 0.5 * across
    return following[:, None], divergence[None]


def solution(mesh):
    placed = (P(None, "gz", None, "pa", None), P("pa", None))
    return jax.shard_map(
        on_device,
        mesh=mesh,
        in_specs=placed,
        out_specs=(P(None, "gz", None, "pa", None), P("gz", None, "pa", None)),
        check_vma=False,
    )
```

```python
import functools
import math

import jax
import jax.numpy as jnp
import ml_dtypes
import numpy as np
from jax import lax
from jax.experimental import pallas as pl
from jax.experimental.pallas import tpu as pltpu
from jax.sharding import PartitionSpec as P

time_step = 0.2
viscosity = 0.25
LANES = 128
HALF = LANES // 2
ROWS = 8
MOST = 16


def halves(table):
    high = table.astype(np.float32).astype(ml_dtypes.bfloat16)
    low = (table - high.astype(np.float64)).astype(np.float32).astype(ml_dtypes.bfloat16)
    return np.stack([high, low])


def wheel(rows, cols, period):
    angle = 2.0 * np.pi / period * (np.outer(rows, cols) % period)
    return np.cos(angle), np.sin(angle)


@functools.lru_cache(maxsize=None)
def tables(ncols, half, lines):
    radix = ncols // LANES
    lane = np.arange(LANES)
    scale = 1.0 / math.sqrt(ncols)
    cos, sin = wheel(lane, lane, LANES)
    forward = np.zeros((2 * LANES, 2 * LANES))
    for part in range(LANES // lines):
        x2 = np.arange(part * lines, (part + 1) * lines)
        at = part * 2 * lines
        forward[:LANES, at : at + lines] = cos[:, x2]
        forward[LANES:, at : at + lines] = -sin[:, x2]
        forward[:LANES, at + lines : at + 2 * lines] = sin[:, x2]
        forward[LANES:, at + lines : at + 2 * lines] = cos[:, x2]
    backward = forward.T
    turn_cos, turn_sin = wheel(np.arange(radix), lane, ncols)
    turns = np.concatenate([turn_cos, turn_sin]).astype(np.float32)
    quarter = half // 2
    nrows = 2 * half
    b = np.arange(quarter)
    yscale = 1.0 / math.sqrt(nrows)
    ycos, ysin = wheel(b, b, quarter)
    to_grid = 2.0 * yscale * np.concatenate([ycos, -ysin], 1)
    from_grid = yscale * np.concatenate([ycos, -ysin], 0)
    column = np.zeros((quarter, LANES))
    for y1 in range(1, 4):
        c, s = wheel(b, np.array([y1]), nrows)
        column[:, 2 * y1] = c[:, 0]
        column[:, 2 * y1 + 1] = s[:, 0]
    modes = np.arange(ncols)
    signed = np.where(modes < ncols // 2, modes, modes - ncols).astype(np.float32)
    wave = np.broadcast_to(np.float32(2.0 * math.pi / ncols) * signed, (ROWS, ncols))
    return dict(
        forward=halves(forward * scale),
        backward=halves(backward * scale),
        turns=turns,
        to_grid=halves(to_grid),
        from_grid=halves(from_grid),
        column=column.astype(np.float32),
        wave=np.ascontiguousarray(wave),
    )


def split(value):
    high = value.astype(jnp.bfloat16)
    low = (value - high.astype(jnp.float32)).astype(jnp.bfloat16)
    return high, low


def product(a_high, a_low, b_high, b_low):
    dot = functools.partial(jnp.dot, preferred_element_type=jnp.float32)
    return dot(a_high, b_low) + dot(a_low, b_high) + dot(a_high, b_high)


def butterfly(terms, sign):
    count = len(terms)
    if count == 1:
        return terms
    even = butterfly(terms[0::2], sign)
    odd = butterfly(terms[1::2], sign)
    first, second = [], []
    for k in range(count // 2):
        real, imag = odd[k]
        if k == 0:
            pass
        elif 4 * k == count:
            real, imag = -sign * imag, sign * real
        elif 8 * k == count:
            root = math.sqrt(0.5)
            real, imag = root * (real - sign * imag), root * (imag + sign * real)
        elif 8 * k == 3 * count:
            root = math.sqrt(0.5)
            real, imag = -root * (real + sign * imag), root * (sign * real - imag)
        else:
            c = math.cos(2.0 * math.pi * k / count)
            s = sign * math.sin(2.0 * math.pi * k / count)
            real, imag = c * real - s * imag, s * real + c * imag
        first.append((even[k][0] + real, even[k][1] + imag))
        second.append((even[k][0] - real, even[k][1] - imag))
    return first + second


def scatter(order_ref, all_ref, out_refs):
    if len(out_refs) == 1:
        out_refs[0][...] = all_ref[...]
        return
    for k, out_ref in enumerate(out_refs):
        out_ref[...] = all_ref[order_ref[k]]


def collect(order_ref, in_refs, all_ref):
    if len(in_refs) == 1:
        all_ref[...] = in_refs[0][...]
        return
    for k, in_ref in enumerate(in_refs):
        all_ref[order_ref[k]] = in_ref[...]


def x_forward_kernel(order_ref, vel_hbm, wave_hbm, turn_hbm, mat_hbm, *rest):
    out_refs = rest[:-7]
    vel_ref, wave_ref, turn_ref, mat_ref, mid_ref, all_ref, sems = rest[-7:]
    kyl, ncols = vel_ref.shape[2:]
    radix = ncols // LANES
    moves = ((vel_hbm, vel_ref), (wave_hbm, wave_ref), (turn_hbm, turn_ref), (mat_hbm, mat_ref))
    copies = [pltpu.make_async_copy(src, dst, sems.at[i]) for i, (src, dst) in enumerate(moves)]
    for copy in copies:
        copy.start()
    for copy in copies:
        copy.wait()

    def chunk(c, carry):
        base = pl.multiple_of(c * ROWS, ROWS)
        rows = pl.ds(base, ROWS)

        def emit(field, terms):
            for x1, (real, imag) in enumerate(butterfly(terms, 1.0)):
                if x1:
                    cos = turn_ref[x1 : x1 + 1, :]
                    sin = turn_ref[radix + x1 : radix + x1 + 1, :]
                    real, imag = real * cos - imag * sin, real * sin + imag * cos
                at = pl.ds(pl.multiple_of(field * kyl + base, ROWS), ROWS)
                mid_ref[x1, at, 0:LANES] = real
                mid_ref[x1, at, LANES : 2 * LANES] = imag

        def load(field):
            cols = [slice(a * LANES, (a + 1) * LANES) for a in range(radix)]
            return [(vel_ref[field, 0, rows, s], vel_ref[field, 1, rows, s]) for s in cols]

        def slope(terms):
            waves = [wave_ref[:, a * LANES : (a + 1) * LANES] for a in range(radix)]
            return [(-k * imag, k * real) for k, (real, imag) in zip(waves, terms)]

        emit(0, load(0))
        emit(1, load(1))
        emit(2, load(2))
        emit(3, slope(load(2)))
        emit(4, slope(load(1)))
        return carry

    lax.fori_loop(0, kyl // ROWS, chunk, 0)
    for x1 in range(radix):
        high, low = split(mid_ref[x1])
        lines = product(high, low, mat_ref[0], mat_ref[1])
        all_ref[2 * x1] = lines[:, :LANES]
        all_ref[2 * x1 + 1] = lines[:, LANES:]
    scatter(order_ref, all_ref, out_refs)


def grid_kernel(count, outs, order_ref, *rest):
    wall_in, to_ref, from_ref, column_ref = rest[count : count + 4]
    out_refs = rest[count + 4 : count + 4 + outs]
    high_ref, low_ref, back_high, back_low, recv_ref, out_ref, wall_ref = rest[count + 4 + outs :]
    collect(order_ref, rest[:count], recv_ref)
    collect(order_ref, [wall_in.at[k] for k in range(count)] if count > 1 else [wall_in], wall_ref)
    groups = recv_ref.shape[0]
    kyl = recv_ref.shape[1] // 5
    quarter = groups * kyl // 2
    block = 32
    each = block // kyl
    gap = groups // 2
    ky_step = 2.0 * math.pi / (4 * quarter)
    left = lax.broadcasted_iota(jnp.int32, (block, LANES), 1) < HALF
    swap = lambda value: pltpu.roll(value, HALF, 1)

    def fields(first, row):
        sources = pl.ds(first, each)
        load = lambda ref, f: ref[sources, f * kyl : (f + 1) * kyl, :].reshape(block, LANES)

        index = row + lax.broadcasted_iota(jnp.int32, (block, LANES), 0)
        ky = index.astype(jnp.float32) * ky_step
        weight = jnp.where(index == 0, 0.5, 1.0)
        ky_signed = jnp.where(left, -ky, ky)
        u, v, w, dw, dv = [load(recv_ref, f) for f in range(5)]
        du_dz, dv_dz = load(wall_ref, 0), load(wall_ref, 1)
        omega_x = ky_signed * swap(w) - dv_dz
        omega_y = du_dz - dw
        omega_z = dv - ky_signed * swap(u)
        result = []
        for one, two in ((u, v), (omega_x, omega_y), (w, omega_z)):
            one = one * weight
            two = two * weight
            result.append((jnp.where(left, one, swap(two)), jnp.where(left, swap(one), two)))
        return result

    def column(rows, k):
        return jnp.broadcast_to(column_ref[rows, k : k + 1], (block, LANES))

    def load_block(c, carry):
        base = pl.multiple_of(c * block, block)
        rows = pl.ds(base, block)
        near = fields(c * each, base)
        far = fields(c * each + gap, base + quarter)
        for pair in range(3):
            a_re, a_im = near[pair]
            b_re, b_im = far[pair]
            sums = (
                (a_re + b_re, a_im + b_im),
                (a_re - b_im, a_im + b_re),
                (a_re - b_re, a_im - b_im),
                (a_re + b_im, a_im - b_re),
            )
            for y1, (real, imag) in enumerate(sums):
                if y1:
                    cos = column(rows, 2 * y1)
                    sin = column(rows, 2 * y1 + 1)
                    real, imag = real * cos - imag * sin, real * sin + imag * cos
                at = slice((3 * y1 + pair) * LANES, (3 * y1 + pair + 1) * LANES)
                lower = pl.ds(pl.multiple_of(quarter + base, block), block)
                high_ref[rows, at], low_ref[rows, at] = split(real)
                high_ref[lower, at], low_ref[lower, at] = split(imag)
        return carry

    lax.fori_loop(0, quarter // block, load_block, 0)

    wide = lax.broadcasted_iota(jnp.int32, (quarter, LANES), 1) < HALF
    kept = None
    for y1 in range(4):
        at = slice(3 * y1 * LANES, 3 * (y1 + 1) * LANES)
        grid = product(to_ref[0], to_ref[1], high_ref[:, at], low_ref[:, at])
        uv = grid[:, :LANES]
        xy = grid[:, LANES : 2 * LANES]
        wz = grid[:, 2 * LANES :]
        zw = swap(wz)
        h_yx = jnp.where(wide, wz, zw) * xy - jnp.where(wide, zw, wz) * uv
        spin = uv * swap(xy)
        h_z = spin - swap(spin)
        slot = slice(y1 * LANES, (y1 + 1) * LANES)
        back_high[:, slot], back_low[:, slot] = split(h_yx)
        if y1 % 2 == 0:
            kept = h_z
        else:
            slot = slice((4 + y1 // 2) * LANES, (5 + y1 // 2) * LANES)
            back_high[:, slot], back_low[:, slot] = split(jnp.where(wide, kept, -h_z))

    freq = product(from_ref[0], from_ref[1], back_high[...], back_low[...])

    column_all = lambda k: jnp.broadcast_to(column_ref[:, k : k + 1], (quarter, LANES))

    def piece(slot, cos, sin):
        real = freq[:quarter, slot * LANES : (slot + 1) * LANES]
        imag = freq[quarter:, slot * LANES : (slot + 1) * LANES]
        if cos is None:
            return real, imag
        return real * cos + imag * sin, imag * cos - real * sin

    turn = [(None, None)] + [(column_all(2 * y1), column_all(2 * y1 + 1)) for y1 in range(1, 4)]
    one = jnp.ones((quarter, LANES), jnp.float32)
    zero = jnp.zeros((quarter, LANES), jnp.float32)
    q0, q1, q2, q3 = [piece(y1, *turn[y1]) for y1 in range(4)]
    z01 = piece(4, jnp.where(wide, one, turn[1][0]), jnp.where(wide, zero, turn[1][1]))
    z23 = piece(5, jnp.where(wide, turn[2][0], turn[3][0]), jnp.where(wide, turn[2][1], turn[3][1]))
    near_re = q0[0] + q1[0] + q2[0] + q3[0]
    near_im = q0[1] + q1[1] + q2[1] + q3[1]
    far_re = q0[0] + q1[1] - q2[0] - q3[1]
    far_im = q0[1] - q1[0] - q2[1] + q3[0]
    v_re, v_im = z01[0] + z23[0], z01[1] + z23[1]
    z_near = jnp.where(wide, v_re + swap(v_re), v_im + swap(v_im))
    d_re, d_im = z01[0] - z23[0], z01[1] - z23[1]
    z_far = jnp.where(wide, d_re + swap(d_im), swap(d_im) - d_re)

    def store(first, field, value):
        for s in range(gap):
            out_ref[first + s, field * kyl : (field + 1) * kyl, :] = value[s * kyl : (s + 1) * kyl]

    for first, real, imag, h_z in ((0, near_re, near_im, z_near), (gap, far_re, far_im, z_far)):
        store(first, 0, -jnp.where(wide, swap(real), imag))
        store(first, 1, jnp.where(wide, real, swap(imag)))
        store(first, 2, h_z)
    scatter(order_ref, out_ref, out_refs)


def x_backward_kernel(count, order_ref, *rest):
    vel_ref, side_ref, mask_ref, ky_ref, wave_ref, turn_ref, mat_ref, next_ref, div_ref, w_ref, mid_ref, recv_ref = rest[count:]
    collect(order_ref, rest[:count], recv_ref)
    kyl, ncols = vel_ref.shape[2:]
    radix = ncols // LANES
    for x1 in range(radix):
        high, low = split(jnp.concatenate([recv_ref[2 * x1], recv_ref[2 * x1 + 1]], axis=1))
        freq = product(high, low, mat_ref[0], mat_ref[1])
        real = freq[:, :LANES]
        imag = freq[:, LANES:]
        if x1:
            cos = turn_ref[x1 : x1 + 1, :]
            sin = turn_ref[radix + x1 : radix + x1 + 1, :]
            real, imag = real * cos + imag * sin, imag * cos - real * sin
        mid_ref[x1, :, 0:LANES] = real
        mid_ref[x1, :, LANES : 2 * LANES] = imag

    def chunk(c, carry):
        base = pl.multiple_of(c * ROWS, ROWS)
        rows = pl.ds(base, ROWS)
        ky = ky_ref[rows, :]
        for field in range(3):
            at = pl.ds(pl.multiple_of(field * kyl + base, ROWS), ROWS)
            terms = [(mid_ref[x1, at, 0:LANES], mid_ref[x1, at, LANES : 2 * LANES]) for x1 in range(radix)]
            for a, pair in enumerate(butterfly(terms, -1.0)):
                cols = slice(a * LANES, (a + 1) * LANES)
                kx = wave_ref[:, cols]
                keep = mask_ref[rows, cols] != 0
                decay = viscosity * (2.0 + kx * kx + ky * ky)
                fresh = []
                for part in range(2):
                    speed = vel_ref[field, part, rows, cols]
                    change = jnp.where(keep, pair[part], 0.0)
                    change = change + viscosity * side_ref[field, part, rows, cols] - decay * speed
                    fresh.append(speed + time_step * change)
                    next_ref[field, part, rows, cols] = fresh[part]
                if field == 0:
                    div_ref[0, rows, cols] = -kx * fresh[1]
                    div_ref[1, rows, cols] = kx * fresh[0]
                elif field == 1:
                    div_ref[0, rows, cols] = div_ref[0, rows, cols] - ky * fresh[1]
                    div_ref[1, rows, cols] = div_ref[1, rows, cols] + ky * fresh[0]
                else:
                    w_ref[0, rows, cols] = fresh[0]
                    w_ref[1, rows, cols] = fresh[1]
        return carry

    lax.fori_loop(0, kyl // ROWS, chunk, 0)


def neighbours(block, axis):
    count = lax.axis_size(axis)
    if count == 1:
        return jnp.zeros_like(block), jnp.zeros_like(block)
    if count == 2:
        other = lax.ppermute(block, axis, [(0, 1), (1, 0)])
        sign = jnp.where(lax.axis_index(axis) == 0, 1.0, -1.0).astype(jnp.float32)
        return other, sign * other
    forward = [(i, i + 1) for i in range(count - 1)]
    below = lax.ppermute(block, axis, forward)
    above = lax.ppermute(block, axis, [(j, i) for i, j in forward])
    return above + below, above - below


def call(kernel, out, scratch, *args, hbm=()):
    whole = pl.BlockSpec(memory_space=pltpu.VMEM)
    spec = {0: pl.BlockSpec(memory_space=pltpu.SMEM)}
    spec.update({i: pl.BlockSpec(memory_space=pltpu.HBM) for i in hbm})
    return pl.pallas_call(
        kernel,
        in_specs=[spec.get(i, whole) for i in range(len(args))],
        out_shape=out,
        scratch_shapes=scratch,
        compiler_params=pltpu.CompilerParams(vmem_limit_bytes=40 * 2**20),
    )(*args)


def on_device(velocity, mode_mask):
    groups = lax.axis_size("pa")
    rank = lax.axis_index("pa")
    depth, kyl, ncols = velocity.shape[1], velocity.shape[3], velocity.shape[4]
    assert depth == 1
    lines = ncols // groups
    half = kyl * groups
    radix = ncols // LANES
    quarter = half // 2
    pieces = HALF // lines
    table = tables(ncols, half, lines)
    f32 = functools.partial(jax.ShapeDtypeStruct, dtype=jnp.float32)
    bf16 = jnp.bfloat16
    speed = velocity[:, 0]
    side, _ = neighbours(speed, "gz")

    direct = pieces == 1 and lines == HALF and groups & (groups - 1) == 0 and groups <= MOST
    steps = [0] + list(reversed(range(1, groups)))
    order = jnp.bitwise_xor(rank, jnp.array(steps, dtype=jnp.int32)).astype(jnp.int32)

    def exchange(blocks):
        if not direct:
            return [lax.all_to_all(blocks[0], "pa", split_axis=0, concat_axis=0, tiled=True)]
        moved = [blocks[0]]
        for block, k in zip(blocks[1:], steps[1:]):
            moved.append(lax.ppermute(block, "pa", [(i, i ^ k) for i in range(groups)]))
        return moved

    def exchange_whole(block):
        return lax.all_to_all(block, "pa", split_axis=0, concat_axis=0, tiled=True)

    def pieces_of(rows, count):
        if direct:
            return [f32((rows, LANES)) for _ in range(count)]
        return [f32((count, rows, LANES))]

    def deal(block):
        if pieces == 1:
            return block
        count, rows, _ = block.shape
        block = block.reshape(count, rows, pieces, 2 * lines)
        return jnp.swapaxes(block, 1, 2).reshape(count * pieces, rows, 2 * lines)

    def gather(block):
        if pieces == 1:
            return block
        rows = block.shape[1]
        block = block.reshape(groups // pieces, pieces, rows, 2 * lines)
        return jnp.swapaxes(block, 1, 2).reshape(groups // pieces, rows, LANES)

    def widen(block):
        if lines == HALF:
            return block
        parts = [jnp.pad(p, ((0, 0), (0, 0), (0, HALF - lines))) for p in (block[..., :lines], block[..., lines:])]
        return jnp.concatenate(parts, -1)

    def narrow(block):
        if lines == HALF:
            return block
        return jnp.concatenate([block[..., :lines], block[..., HALF : HALF + lines]], -1)

    here = lambda array: pltpu.VMEM(array.shape, array.dtype)
    count = groups if direct else 1
    sent = call(
        x_forward_kernel,
        pieces_of(5 * kyl, 2 * radix),
        [
            pltpu.VMEM(speed.shape, jnp.float32),
            here(table["wave"]),
            here(table["turns"]),
            here(table["forward"]),
            pltpu.VMEM((radix, 5 * kyl, 2 * LANES), jnp.float32),
            pltpu.VMEM((2 * radix, 5 * kyl, LANES), jnp.float32),
            pltpu.SemaphoreType.DMA((4,)),
        ],
        order,
        speed,
        table["wave"],
        table["turns"],
        table["forward"],
        hbm=(1, 2, 3, 4),
    )
    received = exchange([sent[0] if direct else deal(sent[0])] + list(sent[1:]))
    if direct:
        stacked = jnp.stack([block[: 2 * kyl] for block in received])
    else:
        stacked = received[0][:, : 2 * kyl]
    _, across = neighbours(stacked, "gz")
    sent = call(
        functools.partial(grid_kernel, count, 1),
        [f32((groups, 3 * kyl, LANES))],
        [
            pltpu.VMEM((half, 12 * LANES), bf16),
            pltpu.VMEM((half, 12 * LANES), bf16),
            pltpu.VMEM((quarter, 6 * LANES), bf16),
            pltpu.VMEM((quarter, 6 * LANES), bf16),
            pltpu.VMEM((groups, 5 * kyl, LANES), jnp.float32),
            pltpu.VMEM((groups, 3 * kyl, LANES), jnp.float32),
            pltpu.VMEM((groups, 2 * kyl, LANES), jnp.float32),
        ],
        order,
        *[widen(block) for block in received],
        widen(0.5 * across),
        table["to_grid"],
        table["from_grid"],
        table["column"],
    )
    received = [gather(exchange_whole(narrow(sent[0])))]
    own_modes = rank * kyl + jnp.arange(kyl, dtype=jnp.int32)
    ky = (2.0 * math.pi / (2 * half)) * own_modes.astype(jnp.float32)
    following, partial, w_next = call(
        functools.partial(x_backward_kernel, 1),
        (f32(speed.shape), f32(speed.shape[1:]), f32(speed.shape[1:])),
        [
            pltpu.VMEM((radix, 3 * kyl, 2 * LANES), jnp.float32),
            pltpu.VMEM((2 * radix, 3 * kyl, LANES), jnp.float32),
        ],
        order,
        *received,
        speed,
        side,
        mode_mask,
        jnp.broadcast_to(ky[:, None], (kyl, LANES)),
        table["wave"],
        table["turns"],
        table["backward"],
    )
    _, across = neighbours(w_next, "gz")
    divergence = partial + 0.5 * across
    return following[:, None], divergence[None]


def solution(mesh):
    placed = (P(None, "gz", None, "pa", None), P("pa", None))
    return jax.shard_map(
        on_device,
        mesh=mesh,
        in_specs=placed,
        out_specs=(P(None, "gz", None, "pa", None), P("gz", None, "pa", None)),
        check_vma=False,
    )
```
